64 devices in a mesh: dp: 8 (over x, y, core), sp: 8 (over z).
Axes of the slice: x: 2, y: 2, z: 8, core: 2. Of those that a mesh axis runs over, the one named last changes fastest.
The devices are a block of a 4x4x8 slice.
Arguments:
- q: bfloat16 [256, 64, 64], P('dp'), parts along dimension 0
- k: bfloat16 [256, 8192, 8, 64], P('dp', 'sp'), parts along dimension 0
- v: bfloat16 [256, 8192, 8, 64], P('dp', 'sp'), parts along dimension 0
Outputs:
- q: bfloat16 [256, 64, 64], P('dp'), parts along dimension 0
There are 8 independent parts. The reference program is written for one: setup_inputs(seed, part) draws one part's arguments, and reference() takes and returns one part's arrays. A program takes and returns all parts, laid end to end along the dimension named above; each array names one.
All inputs are finite; a program needn't handle non-finite values.
Results may differ from the reference program's by a relative error of at most 0.012.
Values are sent between devices in bfloat16 or wider.
A program may use at most 768 MiB of HBM per device.

```python
import jax
import jax.numpy as jnp

BATCH = 32
CACHE = 8192
HEADS = 64
KV_HEADS = 8
HEAD = 64


def setup_inputs(seed: int = 0, part: int = 0) -> dict:
    kq, kk, kv = (jax.random.fold_in(k, part) for k in jax.random.split(jax.random.key(seed), 3))
    return {
        "q": (3 * jax.random.normal(kq, (BATCH, HEADS, HEAD), jnp.float32)).astype(jnp.bfloat16),
        "k": jax.random.normal(kk, (BATCH, CACHE, KV_HEADS, HEAD), jnp.float32).astype(jnp.bfloat16),
        "v": jax.random.normal(kv, (BATCH, CACHE, KV_HEADS, HEAD), jnp.float32).astype(jnp.bfloat16),
    }


def einsum(form, a, b):
    return jnp.einsum(form, a.astype(jnp.float32), b.astype(jnp.float32))


def reference(q, k, v):
    grouped = q.reshape(BATCH, KV_HEADS, -1, HEAD)
    scores = einsum("bgsd,bugd->bgsu", grouped, k) * HEAD**-0.5
    weights = jax.nn.softmax(scores, -1).astype(jnp.bfloat16)
    return einsum("bgsu,bugd->bgsd", weights, v).astype(jnp.bfloat16).reshape(BATCH, HEADS, HEAD)
```

```python
import functools
import math

import jax
import jax.numpy as jnp
from jax import lax
from jax.experimental import pallas as pl
from jax.experimental.pallas import tpu as pltpu
from jax.sharding import PartitionSpec as P

MESH = pl.DeviceIdType.MESH
F32, BF16 = jnp.float32, jnp.bfloat16
SLOTS = 8
LAG = 2


def kernel(n, q_ref, k_ref, v_ref, out_ref, kbuf, vbuf, qq, pbuf, stage, stat, part, parts, stats, result, ksem, vsem, part_send, part_recv, stat_send, stat_recv, res_send, res_recv):
    batch, heads, head = q_ref.shape
    tokens = k_ref.shape[2]
    kv_heads = k_ref.shape[1] // head
    share = heads // kv_heads
    half = kv_heads // 2
    rows = half * share
    wide = half * head
    pairs = batch // 2
    chunks = pairs // 2
    sub = head // n
    scale = head**-0.5 * math.log2(math.e)
    me = lax.axis_index("sp")
    order = [n // 2] + [s for t in range(n // 2 - 1, 0, -1) for s in (t, n - t)]
    peers = [lax.rem(me + t, n) for t in order]

    def fetch(hbm, buf, sem, b):
        slot = lax.rem(b, SLOTS)
        return pltpu.make_async_copy(hbm.at[b], buf.at[slot], sem.at[slot])

    for b in range(SLOTS):
        fetch(k_ref, kbuf, ksem, b).start()
        fetch(v_ref, vbuf, vsem, b).start()

    barrier = pltpu.get_barrier_semaphore()
    for peer in peers:
        pl.semaphore_signal(barrier, inc=1, device_id={"sp": peer}, device_id_type=MESH)

    q = q_ref[...]
    qq[...] = jnp.concatenate([q, q], -1)

    def of(x, c):
        return x.at[c, pl.ds(0, n - 1)]

    def scores(i):
        own = (lax.broadcasted_iota(jnp.int32, (rows, wide), 0) // share) == (lax.broadcasted_iota(jnp.int32, (rows, wide), 1) // head)
        highs, sums = [], []
        for t in range(2):
            b = 2 * i + t
            slot = lax.rem(b, SLOTS)
            fetch(k_ref, kbuf, ksem, b).wait()
            for h in range(2):
                x = qq[b, pl.ds(h * rows, rows), :]
                x = jnp.where(own, jnp.concatenate([x] * (wide // (2 * head)), -1), jnp.zeros((), BF16))
                s = jnp.dot(x, kbuf[slot, pl.ds(h * wide, wide), :], preferred_element_type=F32)
                high = jnp.max(s, -1, keepdims=True)
                w = jnp.exp2((s - high) * scale)
                pbuf[lax.rem(i, 2), t, pl.ds(h * rows, rows), :] = w.astype(BF16)
                highs.append(high)
                sums.append(jnp.sum(w, -1, keepdims=True))
        high, total = jnp.concatenate(highs, 0), jnp.concatenate(sums, 0)
        lane = lax.broadcasted_iota(jnp.int32, (2 * heads, 128), 1)
        stat[i // 2, pl.ds(2 * lax.rem(i, 2), 2), :] = jnp.where(lane == 0, high, total).T[:2]

    def values(i):
        seen = []
        for t in range(2):
            b = 2 * i + t
            slot = lax.rem(b, SLOTS)
            fetch(v_ref, vbuf, vsem, b).wait()
            r = lax.dot_general(vbuf[slot], pbuf[lax.rem(i, 2), t], (((1,), (1,)), ((), ())), preferred_element_type=F32)
            lane = lax.broadcasted_iota(jnp.int32, (head, heads), 1) // share
            o = r[:head]
            for g in range(1, kv_heads):
                o = jnp.where(lane == g, r[g * head : (g + 1) * head], o)
            seen.append(o)
        stage[:, pl.ds(lax.rem(i, 2), 1)] = jnp.concatenate(seen, 1).reshape(n, 1, sub, 2 * heads)

    def send(c):
        part[c] = stage[...].reshape(n, 2 * sub, 2 * heads).astype(BF16)
        parts[c, me] = part[c, me]
        stats[c, me] = stat[c]
        for peer in peers:
            pltpu.make_async_remote_copy(stat.at[c], stats.at[c, me], stat_send.at[c], stat_recv.at[c], device_id={"sp": peer}, device_id_type=MESH).start()
            pltpu.make_async_remote_copy(part.at[c, peer], parts.at[c, me], part_send.at[c], part_recv.at[c], device_id={"sp": peer}, device_id_type=MESH).start()

    def wait_recv(x, c, send_sem, recv_sem):
        pltpu.make_async_remote_copy(of(x, c), of(x, c), send_sem.at[c], recv_sem.at[c], device_id={"sp": peers[0]}, device_id_type=MESH).wait_recv()

    def wait_send(x, c, send_sem, recv_sem):
        pltpu.make_async_remote_copy(of(x, c), of(x, c), send_sem.at[c], recv_sem.at[c], device_id={"sp": peers[0]}, device_id_type=MESH).wait_send()

    def combine(c):
        wait_recv(stats, c, stat_send, stat_recv)
        wait_recv(parts, c, part_send, part_recv)
        highs = [stats[c, d, pl.ds(0, 4), :] for d in range(n)]
        top = functools.reduce(jnp.maximum, highs)
        top_of = [jnp.broadcast_to(top[2 * p : 2 * p + 1], (sub, 2 * heads)) for p in range(2)]
        acc, total = [0.0, 0.0], [0.0, 0.0]
        for d in range(n):
            x = parts[c, d].astype(F32)
            for p in range(2):
                e = jnp.exp2((highs[d][2 * p : 2 * p + 1] - top_of[p]) * scale)
                acc[p] += x[p * sub : (p + 1) * sub] * e
                total[p] += highs[d][2 * p + 1 : 2 * p + 2] * e
        result[c, me] = jnp.concatenate([acc[p] / total[p] for p in range(2)], 0).astype(BF16)
        for peer in peers:
            pltpu.make_async_remote_copy(result.at[c, me], result.at[c, me], res_send.at[c], res_recv.at[c], device_id={"sp": peer}, device_id_type=MESH).start()

    def finish(c):
        wait_recv(result, c, res_send, res_recv)
        x = result[c].astype(F32)
        for p in range(2):
            y = x[:, p * sub : (p + 1) * sub].reshape(head, 2 * heads).T.astype(BF16)
            out_ref[pl.ds(4 * c + 2 * p, 2)] = y.reshape(2, heads, head)

    def refill(hbm, buf, sem, i):
        @pl.when(2 * i < batch)
        def _():
            for t in range(2):
                fetch(hbm, buf, sem, 2 * i + t).start()

    scores(0)
    refill(k_ref, kbuf, ksem, SLOTS // 2)
    pl.semaphore_wait(barrier, n - 1)

    def after(i):
        c = i // 2

        @pl.when(lax.rem(i, 2) == 1)
        def _():
            send(c)

            @pl.when(c >= LAG)
            def _():
                combine(c - LAG)

            @pl.when(c >= 2 * LAG)
            def _():
                finish(c - 2 * LAG)

    def step(i, carry):
        scores(i + 1)
        values(i)
        refill(k_ref, kbuf, ksem, i + 1 + SLOTS // 2)
        refill(v_ref, vbuf, vsem, i + SLOTS // 2)
        after(i)
        return carry

    lax.fori_loop(0, pairs - 1, step, 0)
    values(pairs - 1)
    after(jnp.int32(pairs - 1))
    for c in range(chunks - LAG, chunks):
        combine(c)
    for c in range(max(chunks - 2 * LAG, 0), chunks):
        finish(c)
    for c in range(chunks):
        wait_send(parts, c, part_send, part_recv)
        wait_send(stats, c, stat_send, stat_recv)
        wait_send(result, c, res_send, res_recv)


def solution(mesh):
    n = mesh.shape["sp"]

    def step(q, k, v):
        batch, heads, head = q.shape
        _, tokens, kv_heads, _ = k.shape
        k = k.transpose(0, 2, 3, 1).reshape(batch, kv_heads * head, tokens)
        v = v.transpose(0, 2, 3, 1).reshape(batch, kv_heads * head, tokens)
        chunks, sub = batch // 4, head // n
        dma = pltpu.SemaphoreType.DMA
        return pl.pallas_call(
            functools.partial(kernel, n),
            out_shape=jax.ShapeDtypeStruct(q.shape, BF16),
            in_specs=[pl.BlockSpec(memory_space=pltpu.VMEM), pl.BlockSpec(memory_space=pl.ANY), pl.BlockSpec(memory_space=pl.ANY)],
            out_specs=pl.BlockSpec(memory_space=pltpu.VMEM),
            scratch_shapes=[
                pltpu.VMEM((SLOTS, kv_heads * head, tokens), BF16),
                pltpu.VMEM((SLOTS, kv_heads * head, tokens), BF16),
                pltpu.VMEM((batch, heads, 2 * head), BF16),
                pltpu.VMEM((2, 2, heads, tokens), BF16),
                pltpu.VMEM((n, 2, sub, 2 * heads), F32),
                pltpu.VMEM((chunks, 8, 2 * heads), F32),
                pltpu.VMEM((chunks, n, 2 * sub, 2 * heads), BF16),
                pltpu.VMEM((chunks, n, 2 * sub, 2 * heads), BF16),
                pltpu.VMEM((chunks, n, 8, 2 * heads), F32),
                pltpu.VMEM((chunks, n, 2 * sub, 2 * heads), BF16),
                dma((SLOTS,)),
                dma((SLOTS,)),
            ]
            + [dma((chunks,))] * 6,
            compiler_params=pltpu.CompilerParams(collective_id=0, has_side_effects=True, vmem_limit_bytes=60 * 2**20),
        )(q, k, v)

    return jax.shard_map(
        step,
        mesh=mesh,
        in_specs=(P("dp", None, None), P("dp", "sp", None, None), P("dp", "sp", None, None)),
        out_specs=P("dp", None, None),
        check_vma=False,
    )
```

```python
import functools
import math

import jax
import jax.numpy as jnp
from jax import lax
from jax.experimental import pallas as pl
from jax.experimental.pallas import tpu as pltpu
from jax.sharding import PartitionSpec as P

MESH = pl.DeviceIdType.MESH
F32, BF16 = jnp.float32, jnp.bfloat16
TILE = 256
SLOTS = 8
LAG = 3


def kernel(n, q_ref, k_ref, v_ref, out_ref, qbuf, kbuf, vbuf, qq, sbuf, pbuf, stage, stat, part, parts, stats, result, qsem, ksem, vsem, part_send, part_recv, stat_send, stat_recv, res_send, res_recv):
    batch, heads, head = q_ref.shape
    tokens = k_ref.shape[2]
    kv_heads = k_ref.shape[1] // head
    share = heads // kv_heads
    half = kv_heads // 2
    rows = half * share
    wide = half * head
    pairs = batch // 2
    chunks = pairs // 2
    sub = head // n
    scale = head**-0.5 * math.log2(math.e)
    me = lax.axis_index("sp")
    order = [n // 2] + [s for t in range(n // 2 - 1, 0, -1) for s in (t, n - t)]
    peers = [lax.rem(me + t, n) for t in order]

    def fetch(hbm, buf, sem, b):
        slot = lax.rem(b, SLOTS)
        return pltpu.make_async_copy(hbm.at[b], buf.at[slot], sem.at[slot])

    keys, vals = (k_ref, kbuf, ksem), (v_ref, vbuf, vsem)

    def start(x, i):
        for t in range(2):
            fetch(*x, 2 * i + t).start()

    def wait(x, i):
        for t in range(2):
            fetch(*x, 2 * i + t).wait()

    def refill(x, i):
        @pl.when(i < pairs)
        def _():
            start(x, i)

    ahead = SLOTS // 2


    start(keys, 0)
    start(keys, 1)
    start(vals, 0)
    start(keys, 2)
    start(vals, 1)

    barrier = pltpu.get_barrier_semaphore()
    for peer in peers:
        pl.semaphore_signal(barrier, inc=1, device_id={"sp": peer}, device_id_type=MESH)


    q = q_ref[...]
    qq[...] = jnp.concatenate([q, q], -1)

    def of(x, c):
        return x.at[c, pl.ds(0, n - 1)]

    def query(i):
        own = (lax.broadcasted_iota(jnp.int32, (rows, wide), 0) // share) == (lax.broadcasted_iota(jnp.int32, (rows, wide), 1) // head)
        x = []
        for t in range(2):
            for h in range(2):
                y = qq[2 * i + t, pl.ds(h * rows, rows), :]
                x.append(jnp.where(own, jnp.concatenate([y] * (wide // (2 * head)), -1), jnp.zeros((), BF16)))
        return x

    def weigh(i, side):
        highs, sums = [], []
        for t in range(2):
            for h in range(2):
                x = sbuf[side, t, pl.ds(h * rows, rows), :]
                high = jnp.max(x, -1, keepdims=True)
                w = jnp.exp2((x - high) * scale)
                pbuf[side, t, pl.ds(h * rows, rows), :] = w.astype(BF16)
                highs.append(high)
                sums.append(jnp.sum(w, -1, keepdims=True))
        high, total = jnp.concatenate(highs, 0), jnp.concatenate(sums, 0)
        lane = lax.broadcasted_iota(jnp.int32, (2 * heads, 128), 1)
        stat[i // 2, pl.ds(2 * side, 2), :] = jnp.where(lane == 0, high, total).T[:2]

    steps = tokens // TILE

    def block(i, side, scores, weights, values):
        if weights:
            weigh(i + 1, 1 - side)
        if scores:
            x = query(i + 2)
        seen = [[None, None], [None, None]]
        for h in range(2):
            for c in range(steps):
                for t in range(2):
                    if values:
                        a = vbuf[lax.rem(2 * i + t, SLOTS), pl.ds(h * wide, wide), pl.ds(c * TILE, TILE)]
                        p = pbuf[side, t, pl.ds(h * rows, rows), pl.ds(c * TILE, TILE)]
                        d = lax.dot_general(a, p, (((1,), (1,)), ((), ())), preferred_element_type=F32)
                        seen[t][h] = d if c == 0 else seen[t][h] + d
                    if scores:
                        y = kbuf[lax.rem(2 * i + 4 + t, SLOTS), pl.ds(h * wide, wide), pl.ds(c * TILE, TILE)]
                        sbuf[side, t, pl.ds(h * rows, rows), pl.ds(c * TILE, TILE)] = jnp.dot(x[2 * t + h], y, preferred_element_type=F32)
        if values:
            lane = lax.broadcasted_iota(jnp.int32, (head, rows), 1) // share
            own = []
            for t in range(2):
                for h in range(2):
                    o = seen[t][h][:head]
                    for g in range(1, half):
                        o = jnp.where(lane == g, seen[t][h][g * head : (g + 1) * head], o)
                    own.append(o)
            stage[:, side] = jnp.concatenate(own, 1).reshape(n, sub, 2 * heads)

    def send(c):
        part[c] = stage[...].reshape(n, 2 * sub, 2 * heads).astype(BF16)
        parts[c, me] = part[c, me]
        stats[c, me] = stat[c]
        for peer in peers:
            pltpu.make_async_remote_copy(stat.at[c], stats.at[c, me], stat_send.at[c], stat_recv.at[c], device_id={"sp": peer}, device_id_type=MESH).start()
            pltpu.make_async_remote_copy(part.at[c, peer], parts.at[c, me], part_send.at[c], part_recv.at[c], device_id={"sp": peer}, device_id_type=MESH).start()

    def wait_recv(x, c, send_sem, recv_sem):
        pltpu.make_async_remote_copy(of(x, c), of(x, c), send_sem.at[c], recv_sem.at[c], device_id={"sp": peers[0]}, device_id_type=MESH).wait_recv()

    def wait_send(x, c, send_sem, recv_sem):
        pltpu.make_async_remote_copy(of(x, c), of(x, c), send_sem.at[c], recv_sem.at[c], device_id={"sp": peers[0]}, device_id_type=MESH).wait_send()

    def combine(c):
        wait_recv(stats, c, stat_send, stat_recv)
        wait_recv(parts, c, part_send, part_recv)
        highs = [stats[c, d] for d in range(n)]
        top = functools.reduce(jnp.maximum, highs)
        top_of = [jnp.broadcast_to(top[2 * p : 2 * p + 1], (sub, 2 * heads)) for p in range(2)]
        acc, total = [0.0, 0.0], [0.0, 0.0]
        for d in range(n):
            x = parts[c, d].astype(F32)
            for p in range(2):
                e = jnp.exp2((highs[d][2 * p : 2 * p + 1] - top_of[p]) * scale)
                acc[p] += x[p * sub : (p + 1) * sub] * e
                total[p] += highs[d][2 * p + 1 : 2 * p + 2] * e
        result[c, me] = jnp.concatenate([acc[p] / total[p] for p in range(2)], 0).astype(BF16)
        for peer in peers:
            pltpu.make_async_remote_copy(result.at[c, me], result.at[c, me], res_send.at[c], res_recv.at[c], device_id={"sp": peer}, device_id_type=MESH).start()

    def finish(c):
        wait_recv(result, c, res_send, res_recv)
        x = result[c].astype(F32)
        for p in range(2):
            y = x[:, p * sub : (p + 1) * sub].reshape(head, 2 * heads).T.astype(BF16)
            out_ref[pl.ds(4 * c + 2 * p, 2)] = y.reshape(2, heads, head)

    wait(keys, 0)
    block(-2, 0, True, False, False)
    start(keys, 3)
    start(vals, 2)
    wait(keys, 1)
    block(-1, 1, True, True, False)
    start(keys, 4)
    start(vals, 3)
    start(keys, 5)
    pl.semaphore_wait(barrier, n - 1)

    def step(c, carry):
        for side in range(2):
            i = 2 * c + side
            wait(keys, i + 2)
            wait(vals, i)
            block(i, side, True, True, True)
            refill(keys, i + 2 + ahead)
            refill(vals, i + ahead)
        send(c)

        @pl.when(c >= LAG)
        def _():
            combine(c - LAG)

        @pl.when(c >= 2 * LAG)
        def _():
            finish(c - 2 * LAG)

        return carry

    last = chunks - 1
    lax.fori_loop(0, last, step, 0)
    wait(vals, pairs - 2)
    block(pairs - 2, 0, False, True, True)
    wait(vals, pairs - 1)
    block(pairs - 1, 1, False, False, True)
    send(last)
    for c in range(last - LAG, chunks):
        combine(c)
    for c in range(max(last - 2 * LAG, 0), chunks):
        finish(c)
    for c in range(chunks):
        wait_send(parts, c, part_send, part_recv)
        wait_send(stats, c, stat_send, stat_recv)
        wait_send(result, c, res_send, res_recv)


def solution(mesh):
    n = mesh.shape["sp"]

    def step(q, k, v):
        batch, heads, head = q.shape
        _, tokens, kv_heads, _ = k.shape
        k = k.transpose(0, 2, 3, 1).reshape(batch, kv_heads * head, tokens)
        v = v.transpose(0, 2, 3, 1).reshape(batch, kv_heads * head, tokens)
        chunks, sub = batch // 4, head // n
        dma = pltpu.SemaphoreType.DMA
        return pl.pallas_call(
            functools.partial(kernel, n),
            out_shape=jax.ShapeDtypeStruct(q.shape, BF16),
            in_specs=[pl.BlockSpec(memory_space=pltpu.VMEM), pl.BlockSpec(memory_space=pl.ANY), pl.BlockSpec(memory_space=pl.ANY)],
            out_specs=pl.BlockSpec(memory_space=pltpu.VMEM),
            scratch_shapes=[
                pltpu.VMEM(q.shape, BF16),
                pltpu.VMEM((SLOTS, kv_heads * head, tokens), BF16),
                pltpu.VMEM((SLOTS, kv_heads * head, tokens), BF16),
                pltpu.VMEM((batch, heads, 2 * head), BF16),
                pltpu.VMEM((2, 2, heads, tokens), F32),
                pltpu.VMEM((2, 2, heads, tokens), BF16),
                pltpu.VMEM((n, 2, sub, 2 * heads), F32),
                pltpu.VMEM((chunks, 4, 2 * heads), F32),
                pltpu.VMEM((chunks, n, 2 * sub, 2 * heads), BF16),
                pltpu.VMEM((chunks, n, 2 * sub, 2 * heads), BF16),
                pltpu.VMEM((chunks, n, 4, 2 * heads), F32),
                pltpu.VMEM((chunks, n, 2 * sub, 2 * heads), BF16),
                dma,
                dma((SLOTS,)),
                dma((SLOTS,)),
            ]
            + [dma((chunks,))] * 6,
            compiler_params=pltpu.CompilerParams(collective_id=0, has_side_effects=True, vmem_limit_bytes=28 * 2**20),
        )(q, k, v)

    return jax.shard_map(
        step,
        mesh=mesh,
        in_specs=(P("dp", None, None), P("dp", "sp", None, None), P("dp", "sp", None, None)),
        out_specs=P("dp", None, None),
        check_vma=False,
    )
```

```python
import functools
import math

import jax
import jax.numpy as jnp
from jax import lax
from jax.experimental import pallas as pl
from jax.experimental.pallas import tpu as pltpu
from jax.sharding import PartitionSpec as P

MESH = pl.DeviceIdType.MESH
F32, BF16 = jnp.float32, jnp.bfloat16
TILE = 256
SLOTS = 8
LAG = 3
LATE = 2


def kernel(n, q_ref, k_ref, v_ref, out_ref, qbuf, kbuf, vbuf, qq, sbuf, pbuf, stage, stat, part, parts, stats, result, late_stat, late_stats, late, lates, late_result, qsem, ksem, vsem, part_send, part_recv, stat_send, stat_recv, res_send, res_recv, late_stat_send, late_stat_recv, late_send, late_recv, late_res_send, late_res_recv):
    batch, heads, head = q_ref.shape
    tokens = k_ref.shape[2]
    kv_heads = k_ref.shape[1] // head
    share = heads // kv_heads
    half = kv_heads // 2
    rows = half * share
    wide = half * head
    pairs = batch // 2
    chunks = (pairs - LATE) // 2
    owners = n // 2
    sub = head // n
    scale = head**-0.5 * math.log2(math.e)
    me = lax.axis_index("sp")
    order = [n // 2] + [s for t in range(n // 2 - 1, 0, -1) for s in (t, n - t)]
    peers = [lax.rem(me + t, n) for t in order]

    def fetch(hbm, buf, sem, b):
        slot = lax.rem(b, SLOTS)
        return pltpu.make_async_copy(hbm.at[b], buf.at[slot], sem.at[slot])

    keys, vals = (k_ref, kbuf, ksem), (v_ref, vbuf, vsem)

    def start(x, i):
        for t in range(2):
            fetch(*x, 2 * i + t).start()

    def wait(x, i):
        for t in range(2):
            fetch(*x, 2 * i + t).wait()

    ahead = SLOTS // 2

    def more(i):
        @pl.when(i + 2 + ahead < pairs)
        def _():
            start(keys, i + 2 + ahead)

        @pl.when(i + ahead < pairs)
        def _():
            start(vals, i + ahead)

    load_q = pltpu.make_async_copy(q_ref, qbuf, qsem)
    load_q.start()
    start(keys, 0)
    start(keys, 1)
    start(vals, 0)
    for p in range(2, ahead):
        start(keys, p)
        start(vals, p - 1)

    barrier = pltpu.get_barrier_semaphore()
    for peer in peers:
        pl.semaphore_signal(barrier, inc=1, device_id={"sp": peer}, device_id_type=MESH)

    load_q.wait()
    q = qbuf[...]
    qq[...] = jnp.concatenate([q, q], -1)

    def of(x, c):
        return x.at[c, pl.ds(0, n - 1)]

    def query(i):
        own = (lax.broadcasted_iota(jnp.int32, (rows, wide), 0) // share) == (lax.broadcasted_iota(jnp.int32, (rows, wide), 1) // head)
        x = []
        for t in range(2):
            for h in range(2):
                y = qq[2 * i + t, pl.ds(h * rows, rows), :]
                x.append(jnp.where(own, jnp.concatenate([y] * (wide // (2 * head)), -1), jnp.zeros((), BF16)))
        return x

    def weigh(i, side):
        highs, sums = [], []
        for t in range(2):
            for h in range(2):
                x = sbuf[side, t, pl.ds(h * rows, rows), :]
                high = jnp.max(x, -1, keepdims=True)
                w = jnp.exp2((x - high) * scale)
                pbuf[side, t, pl.ds(h * rows, rows), :] = w.astype(BF16)
                highs.append(high)
                sums.append(jnp.sum(w, -1, keepdims=True))
        high, total = jnp.concatenate(highs, 0), jnp.concatenate(sums, 0)
        lane = lax.broadcasted_iota(jnp.int32, (2 * heads, 128), 1)
        stat[i // 2, pl.ds(2 * side, 2), :] = jnp.where(lane == 0, high, total).T[:2]

    steps = tokens // TILE

    def block(i, side, scores, weights, values):
        if weights:
            weigh(i + 1, 1 - side)
        if scores:
            x = query(i + 2)
        seen = [[None, None], [None, None]]
        for h in range(2):
            for c in range(steps):
                for t in range(2):
                    if values:
                        a = vbuf[lax.rem(2 * i + t, SLOTS), pl.ds(h * wide, wide), pl.ds(c * TILE, TILE)]
                        p = pbuf[side, t, pl.ds(h * rows, rows), pl.ds(c * TILE, TILE)]
                        d = lax.dot_general(a, p, (((1,), (1,)), ((), ())), preferred_element_type=F32)
                        seen[t][h] = d if c == 0 else seen[t][h] + d
                    if scores:
                        y = kbuf[lax.rem(2 * i + 4 + t, SLOTS), pl.ds(h * wide, wide), pl.ds(c * TILE, TILE)]
                        sbuf[side, t, pl.ds(h * rows, rows), pl.ds(c * TILE, TILE)] = jnp.dot(x[2 * t + h], y, preferred_element_type=F32)
        if values:
            lane = lax.broadcasted_iota(jnp.int32, (head, rows), 1) // share
            own = []
            for t in range(2):
                for h in range(2):
                    o = seen[t][h][:head]
                    for g in range(1, half):
                        o = jnp.where(lane == g, seen[t][h][g * head : (g + 1) * head], o)
                    own.append(o)
            stage[:, side] = jnp.concatenate(own, 1).reshape(n, sub, 2 * heads)

    def push(src, dst, send_sem, recv_sem, peer):
        pltpu.make_async_remote_copy(src, dst, send_sem, recv_sem, device_id={"sp": peer}, device_id_type=MESH).start()

    def arrive(x, recv_sem):
        pltpu.make_async_remote_copy(x, x, recv_sem, recv_sem, device_id={"sp": peers[0]}, device_id_type=MESH).wait_recv()

    def left(x, send_sem):
        pltpu.make_async_remote_copy(x, x, send_sem, send_sem, device_id={"sp": peers[0]}, device_id_type=MESH).wait_send()

    def weights_of(rows_of, p, size):
        top = functools.reduce(jnp.maximum, [x[2 * p : 2 * p + 1] for x in rows_of])
        e = [jnp.exp2((x[2 * p : 2 * p + 1] - top) * scale) for x in rows_of]
        total = functools.reduce(jnp.add, [x[2 * p + 1 : 2 * p + 2] * y for x, y in zip(rows_of, e)])
        shape = (size, 2 * heads)
        return [jnp.broadcast_to(y, shape) for y in e], jnp.broadcast_to(total, shape)

    def show(b, x):
        out_ref[pl.ds(b, 2)] = x.T.astype(BF16).reshape(2, heads, head)

    def send(c):
        part[c] = stage[...].reshape(n, 2 * sub, 2 * heads).astype(BF16)
        parts[c, me] = part[c, me]
        stats[c, me] = stat[c]
        for peer in peers:
            push(stat.at[c], stats.at[c, me], stat_send.at[c], stat_recv.at[c], peer)
            push(part.at[c, peer], parts.at[c, me], part_send.at[c], part_recv.at[c], peer)

    def combine(c):
        arrive(of(stats, c), stat_recv.at[c])
        arrive(of(parts, c), part_recv.at[c])
        seen = [stats[c, d] for d in range(n)]
        both = []
        x = [parts[c, d].astype(F32) for d in range(n)]
        for p in range(2):
            e, total = weights_of(seen, p, sub)
            both.append(functools.reduce(jnp.add, [x[d][p * sub : (p + 1) * sub] * e[d] for d in range(n)]) / total)
        result[c, me] = jnp.concatenate(both, 0).astype(BF16)
        for peer in peers:
            push(result.at[c, me], result.at[c, me], res_send.at[c], res_recv.at[c], peer)

    def finish(c):
        arrive(of(result, c), res_recv.at[c])
        x = result[c].astype(F32)
        for p in range(2):
            show(4 * c + 2 * p, x[:, p * sub : (p + 1) * sub].reshape(head, 2 * heads))

    mine = lax.rem(me + owners // 2, n)
    owner = mine < owners
    device = [(j + n - owners // 2) % n for j in range(owners)]

    def send_late(e):
        c, side = (pairs - LATE + e) // 2, e % 2
        late_stat[e] = stat[c, pl.ds(2 * side, 2), :]
        late[e] = stage[:, side].reshape(owners, 2 * sub, 2 * heads).astype(BF16)
        for j in range(owners):

            @pl.when(mine != j)
            def _():
                push(late_stat.at[e], late_stats.at[e, me], late_stat_send.at[e], late_stat_recv.at[e], device[j])
                push(late.at[e, j], lates.at[e, me], late_send.at[e], late_recv.at[e], device[j])

            @pl.when(mine == j)
            def _():
                late_stats[e, me] = late_stat[e]
                lates[e, me] = late[e, j]

    def combine_late(e):
        @pl.when(owner)
        def _():
            arrive(of(late_stats, e), late_stat_recv.at[e])
            arrive(of(lates, e), late_recv.at[e])
            w, total = weights_of([late_stats[e, d] for d in range(n)], 0, 2 * sub)
            late_result[e, mine] = (functools.reduce(jnp.add, [lates[e, d].astype(F32) * w[d] for d in range(n)]) / total).astype(BF16)
            for t in range(n - 1):
                peer = t + jnp.where(t >= me, 1, 0)
                push(late_result.at[e, mine], late_result.at[e, mine], late_res_send.at[e], late_res_recv.at[e], peer)

    def finish_late(e):
        @pl.when(owner)
        def _():
            arrive(late_result.at[e, pl.ds(0, owners - 1)], late_res_recv.at[e])

        @pl.when(jnp.logical_not(owner))
        def _():
            arrive(late_result.at[e], late_res_recv.at[e])

        show(batch - 2 * LATE + 2 * e, late_result[e].astype(F32).reshape(head, 2 * heads))

    def leave_late(e):
        @pl.when(owner)
        def _():
            left(late_stats.at[e, pl.ds(0, owners - 1)], late_stat_send.at[e])
            left(lates.at[e, pl.ds(0, owners - 1)], late_send.at[e])
            left(of(lates, e), late_res_send.at[e])

        @pl.when(jnp.logical_not(owner))
        def _():
            left(late_stats.at[e, pl.ds(0, owners)], late_stat_send.at[e])
            left(lates.at[e, pl.ds(0, owners)], late_send.at[e])

    wait(keys, 0)
    block(-2, 0, True, False, False)
    start(keys, ahead)
    start(vals, ahead - 1)
    wait(keys, 1)
    block(-1, 1, True, True, False)
    start(keys, ahead + 1)
    pl.semaphore_wait(barrier, n - 1)

    def step(c, carry):
        for side in range(2):
            i = 2 * c + side
            wait(keys, i + 2)
            wait(vals, i)
            block(i, side, True, True, True)

            more(i)

        send(c)

        @pl.when(c >= LAG)
        def _():
            combine(c - LAG)

        return carry

    lax.fori_loop(0, chunks, step, 0)
    i = pairs - LATE
    wait(vals, i)
    block(i, 0, False, True, True)
    send_late(0)
    wait(vals, i + 1)
    block(i + 1, 1, False, False, True)
    send_late(1)

    def repeat(f, first, end):
        def body(c, carry):
            f(c)
            return carry

        lax.fori_loop(first, end, body, 0)

    def leave(c):
        left(of(parts, c), part_send.at[c])
        left(of(stats, c), stat_send.at[c])
        left(of(result, c), res_send.at[c])

    repeat(combine, chunks - 3, chunks)
    repeat(combine_late, 0, LATE)
    repeat(finish, 0, chunks)
    repeat(finish_late, 0, LATE)
    repeat(leave, 0, chunks)
    repeat(leave_late, 0, LATE)


def solution(mesh):
    n = mesh.shape["sp"]

    def step(q, k, v):
        batch, heads, head = q.shape
        _, tokens, kv_heads, _ = k.shape
        k = k.transpose(0, 2, 3, 1).reshape(batch, kv_heads * head, tokens)
        v = v.transpose(0, 2, 3, 1).reshape(batch, kv_heads * head, tokens)
        chunks, sub = batch // 4 - LATE // 2, head // n
        q = pltpu.with_memory_space_constraint(q, pltpu.HBM)
        dma = pltpu.SemaphoreType.DMA
        return pl.pallas_call(
            functools.partial(kernel, n),
            out_shape=jax.ShapeDtypeStruct(q.shape, BF16),
            in_specs=[pl.BlockSpec(memory_space=pltpu.HBM)] * 3,
            out_specs=pl.BlockSpec(memory_space=pltpu.VMEM),
            scratch_shapes=[
                pltpu.VMEM(q.shape, BF16),
                pltpu.VMEM((SLOTS, kv_heads * head, tokens), BF16),
                pltpu.VMEM((SLOTS, kv_heads * head, tokens), BF16),
                pltpu.VMEM((batch, heads, 2 * head), BF16),
                pltpu.VMEM((2, 2, heads, tokens), F32),
                pltpu.VMEM((2, 2, heads, tokens), BF16),
                pltpu.VMEM((n, 2, sub, 2 * heads), F32),
                pltpu.VMEM((batch // 4, 4, 2 * heads), F32),
                pltpu.VMEM((chunks, n, 2 * sub, 2 * heads), BF16),
                pltpu.VMEM((chunks, n, 2 * sub, 2 * heads), BF16),
                pltpu.VMEM((chunks, n, 4, 2 * heads), F32),
                pltpu.VMEM((chunks, n, 2 * sub, 2 * heads), BF16),
                pltpu.VMEM((LATE, 2, 2 * heads), F32),
                pltpu.VMEM((LATE, n, 2, 2 * heads), F32),
                pltpu.VMEM((LATE, n // 2, 2 * sub, 2 * heads), BF16),
                pltpu.VMEM((LATE, n, 2 * sub, 2 * heads), BF16),
                pltpu.VMEM((LATE, n // 2, 2 * sub, 2 * heads), BF16),
                dma,
                dma((SLOTS,)),
                dma((SLOTS,)),
            ]
            + [dma((chunks,))] * 6
            + [dma((LATE,))] * 6,
            compiler_params=pltpu.CompilerParams(collective_id=0, has_side_effects=True, vmem_limit_bytes=28 * 2**20),
        )(q, k, v)

    return jax.shard_map(
        step,
        mesh=mesh,
        in_specs=(P("dp", None, None), P("dp", "sp", None, None), P("dp", "sp", None, None)),
        out_specs=P("dp", None, None),
        check_vma=False,
    )
```

```python
import functools
import math

import jax
import jax.numpy as jnp
from jax import lax
from jax.experimental import pallas as pl
from jax.experimental.pallas import tpu as pltpu
from jax.sharding import PartitionSpec as P

MESH = pl.DeviceIdType.MESH
F32, BF16 = jnp.float32, jnp.bfloat16
TILE = 256
SLOTS = 6
LAG = 3
LATE = 2


def kernel(n, q_ref, k_ref, v_ref, out_ref, qbuf, kbuf, vbuf, qq, sbuf, pbuf, stage, stat, part, parts, stats, result, late_stat, late_stats, late, lates, late_result, qsem, ksem, vsem, part_send, part_recv, stat_send, stat_recv, res_send, res_recv, late_stat_send, late_stat_recv, late_send, late_recv, late_res_send, late_res_recv):
    batch, heads, head = q_ref.shape
    tokens = k_ref.shape[2]
    kv_heads = k_ref.shape[1] // head
    share = heads // kv_heads
    half = kv_heads // 2
    rows = half * share
    wide = half * head
    pairs = batch // 2
    chunks = (pairs - LATE) // 2
    owners = n // 2
    sub = head // n
    scale = head**-0.5 * math.log2(math.e)
    me = lax.axis_index("sp")
    order = [n // 2] + [s for t in range(n // 2 - 1, 0, -1) for s in (t, n - t)]
    peers = [lax.rem(me + t, n) for t in order]

    def fetch(hbm, buf, sem, b):
        slot = lax.rem(b, SLOTS)
        return pltpu.make_async_copy(hbm.at[b], buf.at[slot], sem.at[slot])

    keys, vals = (k_ref, kbuf, ksem), (v_ref, vbuf, vsem)

    def start(x, i):
        for t in range(2):
            fetch(*x, 2 * i + t).start()

    def wait(x, i):
        for t in range(2):
            fetch(*x, 2 * i + t).wait()

    ahead = SLOTS // 2

    def more(i):
        @pl.when(i + 2 + ahead < pairs)
        def _():
            start(keys, i + 2 + ahead)

        @pl.when(i + ahead < pairs)
        def _():
            start(vals, i + ahead)

    load_q = pltpu.make_async_copy(q_ref, qbuf, qsem)
    load_q.start()
    start(keys, 0)
    start(keys, 1)
    start(vals, 0)
    for p in range(2, ahead):
        start(keys, p)
        start(vals, p - 1)

    barrier = pltpu.get_barrier_semaphore()
    for peer in peers:
        pl.semaphore_signal(barrier, inc=1, device_id={"sp": peer}, device_id_type=MESH)

    load_q.wait()
    q = qbuf[...]
    qq[...] = jnp.concatenate([q, q], -1)

    def of(x, c):
        return x.at[c, pl.ds(0, n - 1)]

    def query(i):
        own = (lax.broadcasted_iota(jnp.int32, (rows, wide), 0) // share) == (lax.broadcasted_iota(jnp.int32, (rows, wide), 1) // head)
        x = []
        for t in range(2):
            for h in range(2):
                y = qq[2 * i + t, pl.ds(h * rows, rows), :]
                x.append(jnp.where(own, jnp.concatenate([y] * (wide // (2 * head)), -1), jnp.zeros((), BF16)))
        return x

    def weigh(i, side):
        highs, sums = [], []
        for t in range(2):
            for h in range(2):
                x = sbuf[side, t, pl.ds(h * rows, rows), :]
                high = jnp.max(x, -1, keepdims=True)
                w = jnp.exp2((x - high) * scale)
                pbuf[side, t, pl.ds(h * rows, rows), :] = w.astype(BF16)
                highs.append(high)
                sums.append(jnp.sum(w, -1, keepdims=True))
        high, total = jnp.concatenate(highs, 0), jnp.concatenate(sums, 0)
        lane = lax.broadcasted_iota(jnp.int32, (2 * heads, 128), 1)
        stat[i // 2, pl.ds(2 * side, 2), :] = jnp.where(lane == 0, high, total).T[:2]

    steps = tokens // TILE

    def block(i, side, scores, weights, values):
        if weights:
            weigh(i + 1, 1 - side)
        if scores:
            x = query(i + 2)
        seen = [[None, None], [None, None]]
        for h in range(2):
            for c in range(steps):
                for t in range(2):
                    if values:
                        a = vbuf[lax.rem(2 * i + t, SLOTS), pl.ds(h * wide, wide), pl.ds(c * TILE, TILE)]
                        p = pbuf[side, t, pl.ds(h * rows, rows), pl.ds(c * TILE, TILE)]
                        d = lax.dot_general(a, p, (((1,), (1,)), ((), ())), preferred_element_type=F32)
                        seen[t][h] = d if c == 0 else seen[t][h] + d
                    if scores:
                        y = kbuf[lax.rem(2 * i + 4 + t, SLOTS), pl.ds(h * wide, wide), pl.ds(c * TILE, TILE)]
                        sbuf[side, t, pl.ds(h * rows, rows), pl.ds(c * TILE, TILE)] = jnp.dot(x[2 * t + h], y, preferred_element_type=F32)
        if values:
            lane = lax.broadcasted_iota(jnp.int32, (head, rows), 1) // share
            own = []
            for t in range(2):
                for h in range(2):
                    o = seen[t][h][:head]
                    for g in range(1, half):
                        o = jnp.where(lane == g, seen[t][h][g * head : (g + 1) * head], o)
                    own.append(o)
            stage[:, side] = jnp.concatenate(own, 1).reshape(n, sub, 2 * heads)

    def push(src, dst, send_sem, recv_sem, peer):
        pltpu.make_async_remote_copy(src, dst, send_sem, recv_sem, device_id={"sp": peer}, device_id_type=MESH).start()

    def arrive(x, recv_sem):
        pltpu.make_async_remote_copy(x, x, recv_sem, recv_sem, device_id={"sp": peers[0]}, device_id_type=MESH).wait_recv()

    def left(x, send_sem):
        pltpu.make_async_remote_copy(x, x, send_sem, send_sem, device_id={"sp": peers[0]}, device_id_type=MESH).wait_send()

    def weights_of(rows_of, p, size):
        top = functools.reduce(jnp.maximum, [x[2 * p : 2 * p + 1] for x in rows_of])
        e = [jnp.exp2((x[2 * p : 2 * p + 1] - top) * scale) for x in rows_of]
        total = functools.reduce(jnp.add, [x[2 * p + 1 : 2 * p + 2] * y for x, y in zip(rows_of, e)])
        shape = (size, 2 * heads)
        return [jnp.broadcast_to(y, shape) for y in e], jnp.broadcast_to(total, shape)

    def show(b, x):
        out_ref[pl.ds(b, 2)] = x.T.astype(BF16).reshape(2, heads, head)

    def send(c):
        part[c] = stage[...].reshape(n, 2 * sub, 2 * heads).astype(BF16)
        parts[c, me] = part[c, me]
        stats[c, me] = stat[c]
        for peer in peers:
            push(stat.at[c], stats.at[c, me], stat_send.at[c], stat_recv.at[c], peer)
            push(part.at[c, peer], parts.at[c, me], part_send.at[c], part_recv.at[c], peer)

    def combine(c):
        arrive(of(stats, c), stat_recv.at[c])
        arrive(of(parts, c), part_recv.at[c])
        seen = [stats[c, d] for d in range(n)]
        both = []
        x = [parts[c, d].astype(F32) for d in range(n)]
        for p in range(2):
            e, total = weights_of(seen, p, sub)
            both.append(functools.reduce(jnp.add, [x[d][p * sub : (p + 1) * sub] * e[d] for d in range(n)]) / total)
        result[c, me] = jnp.concatenate(both, 0).astype(BF16)
        for peer in peers:
            push(result.at[c, me], result.at[c, me], res_send.at[c], res_recv.at[c], peer)

    def finish(c):
        arrive(of(result, c), res_recv.at[c])
        x = result[c].astype(F32)
        for p in range(2):
            show(4 * c + 2 * p, x[:, p * sub : (p + 1) * sub].reshape(head, 2 * heads))

    mine = lax.rem(me + owners // 2, n)
    owner = mine < owners
    device = [(j + n - owners // 2) % n for j in range(owners)]

    def send_late(e):
        c, side = (pairs - LATE + e) // 2, e % 2
        late_stat[e] = stat[c, pl.ds(2 * side, 2), :]
        late[e] = stage[:, side].reshape(owners, 2 * sub, 2 * heads).astype(BF16)
        for j in range(owners):

            @pl.when(mine != j)
            def _():
                push(late_stat.at[e], late_stats.at[e, me], late_stat_send.at[e], late_stat_recv.at[e], device[j])
                push(late.at[e, j], lates.at[e, me], late_send.at[e], late_recv.at[e], device[j])

            @pl.when(mine == j)
            def _():
                late_stats[e, me] = late_stat[e]
                lates[e, me] = late[e, j]

    def combine_late(e):
        @pl.when(owner)
        def _():
            arrive(of(late_stats, e), late_stat_recv.at[e])
            arrive(of(lates, e), late_recv.at[e])
            w, total = weights_of([late_stats[e, d] for d in range(n)], 0, 2 * sub)
            late_result[e, mine] = (functools.reduce(jnp.add, [lates[e, d].astype(F32) * w[d] for d in range(n)]) / total).astype(BF16)
            for t in range(n - 1):
                peer = t + jnp.where(t >= me, 1, 0)
                push(late_result.at[e, mine], late_result.at[e, mine], late_res_send.at[e], late_res_recv.at[e], peer)

    def finish_late(e):
        @pl.when(owner)
        def _():
            arrive(late_result.at[e, pl.ds(0, owners - 1)], late_res_recv.at[e])

        @pl.when(jnp.logical_not(owner))
        def _():
            arrive(late_result.at[e], late_res_recv.at[e])

        show(batch - 2 * LATE + 2 * e, late_result[e].astype(F32).reshape(head, 2 * heads))

    def leave_late(e):
        @pl.when(owner)
        def _():
            left(late_stats.at[e, pl.ds(0, owners - 1)], late_stat_send.at[e])
            left(lates.at[e, pl.ds(0, owners - 1)], late_send.at[e])
            left(of(lates, e), late_res_send.at[e])

        @pl.when(jnp.logical_not(owner))
        def _():
            left(late_stats.at[e, pl.ds(0, owners)], late_stat_send.at[e])
            left(lates.at[e, pl.ds(0, owners)], late_send.at[e])

    wait(keys, 0)
    block(-2, 0, True, False, False)
    start(keys, ahead)
    start(vals, ahead - 1)
    wait(keys, 1)
    block(-1, 1, True, True, False)
    start(keys, ahead + 1)
    pl.semaphore_wait(barrier, n - 1)

    def step(c, carry):
        for side in range(2):
            i = 2 * c + side
            wait(keys, i + 2)
            wait(vals, i)
            block(i, side, True, True, True)

            more(i)

        send(c)

        @pl.when(c >= LAG)
        def _():
            combine(c - LAG)

        return carry

    lax.fori_loop(0, chunks, step, 0)
    i = pairs - LATE
    wait(vals, i)
    block(i, 0, False, True, True)
    send_late(0)
    wait(vals, i + 1)
    block(i + 1, 1, False, False, True)
    send_late(1)

    def repeat(f, first, end):
        def body(c, carry):
            f(c)
            return carry

        lax.fori_loop(first, end, body, 0)

    def leave(c):
        left(of(parts, c), part_send.at[c])
        left(of(stats, c), stat_send.at[c])
        left(of(result, c), res_send.at[c])

    repeat(combine, chunks - 3, chunks)
    repeat(combine_late, 0, LATE)
    repeat(finish, 0, chunks)
    repeat(finish_late, 0, LATE)
    repeat(leave, 0, chunks)
    repeat(leave_late, 0, LATE)


def solution(mesh):
    n = mesh.shape["sp"]

    def step(q, k, v):
        batch, heads, head = q.shape
        _, tokens, kv_heads, _ = k.shape
        k = k.transpose(0, 2, 3, 1).reshape(batch, kv_heads * head, tokens)
        v = v.transpose(0, 2, 3, 1).reshape(batch, kv_heads * head, tokens)
        chunks, sub = batch // 4 - LATE // 2, head // n
        q = pltpu.with_memory_space_constraint(q, pltpu.HBM)
        dma = pltpu.SemaphoreType.DMA
        return pl.pallas_call(
            functools.partial(kernel, n),
            out_shape=jax.ShapeDtypeStruct(q.shape, BF16),
            in_specs=[pl.BlockSpec(memory_space=pltpu.HBM)] * 3,
            out_specs=pl.BlockSpec(memory_space=pltpu.VMEM),
            scratch_shapes=[
                pltpu.VMEM(q.shape, BF16),
                pltpu.VMEM((SLOTS, kv_heads * head, tokens), BF16),
                pltpu.VMEM((SLOTS, kv_heads * head, tokens), BF16),
                pltpu.VMEM((batch, heads, 2 * head), BF16),
                pltpu.VMEM((2, 2, heads, tokens), F32),
                pltpu.VMEM((2, 2, heads, tokens), BF16),
                pltpu.VMEM((n, 2, sub, 2 * heads), F32),
                pltpu.VMEM((batch // 4, 4, 2 * heads), F32),
                pltpu.VMEM((chunks, n, 2 * sub, 2 * heads), BF16),
                pltpu.VMEM((chunks, n, 2 * sub, 2 * heads), BF16),
                pltpu.VMEM((chunks, n, 4, 2 * heads), F32),
                pltpu.VMEM((chunks, n, 2 * sub, 2 * heads), BF16),
                pltpu.VMEM((LATE, 2, 2 * heads), F32),
                pltpu.VMEM((LATE, n, 2, 2 * heads), F32),
                pltpu.VMEM((LATE, n // 2, 2 * sub, 2 * heads), BF16),
                pltpu.VMEM((LATE, n, 2 * sub, 2 * heads), BF16),
                pltpu.VMEM((LATE, n // 2, 2 * sub, 2 * heads), BF16),
                dma,
                dma((SLOTS,)),
                dma((SLOTS,)),
            ]
            + [dma((chunks,))] * 6
            + [dma((LATE,))] * 6,
            compiler_params=pltpu.CompilerParams(collective_id=0, has_side_effects=True, vmem_limit_bytes=28 * 2**20),
        )(q, k, v)

    return jax.shard_map(
        step,
        mesh=mesh,
        in_specs=(P("dp", None, None), P("dp", "sp", None, None), P("dp", "sp", None, None)),
        out_specs=P("dp", None, None),
        check_vma=False,
    )
```
